32 devices in a mesh: io: 16 (over z, x, core), rep: 2 (over y).
Axes of the slice: x: 2, y: 2, z: 4, core: 2. Of those that a mesh axis runs over, the one named last changes fastest.
Arguments:
- snapshots: float32 [49152, 2048], P(('rep', 'io')), parts along dimension 0, may hold values from -6 to 6
Outputs:
- coefficients: float32 [32, 256, 2048], P('rep', None, 'io'), parts along dimension 0
- resid_var: float32 [512, 2048], P('rep', 'io'), parts along dimension 0
The draws below stay inside these ranges and needn't reach their ends.
There are 2 independent parts, one for each index of `rep`. The reference program is written for one: setup_inputs(seed, part) draws one part's arguments, and reference() takes and returns one part's arrays. A program takes and returns all parts, laid end to end along the dimension named above; each array names one. Nothing has to cross between parts.
All inputs are finite; a program needn't handle non-finite values.
Results may differ from the reference program's by a relative error of at most 0.000071.
Values sent between devices are 32-bit elements; how exact they have to be, the bound alone decides.
A program may use at most 128 MiB of HBM per device.

```python
import jax
import jax.numpy as jnp
from jax import lax

TIMES = 96
HARM = 16
LAT = 256
LON = 2048


def level_of(own_key, dims, cuts, low, top_value):
    def one(axis_at, parts):
        heights = jax.random.uniform(jax.random.fold_in(jax.random.fold_in(own_key, 6), axis_at), (parts,), jnp.float32, low / len(cuts), top_value / len(cuts))
        return jnp.repeat(jnp.exp(heights), dims[axis_at] // parts).reshape((-1,) + (1,) * (len(dims) - axis_at - 1))

    gain = one(*cuts[0])
    for cut in cuts[1:]:
        gain = gain * one(*cut)
    return gain


def normal_values(rng, dims, deviation, bound, cuts=(), dtype=jnp.bfloat16):
    array = deviation * jax.random.normal(rng, dims, jnp.float32)
    if cuts:
        array = array * level_of(rng, dims, cuts, -0.22, 0.18)
    return jnp.clip(array, -bound, bound).astype(dtype)


def setup_inputs(seed: int = 0, part: int = 0) -> dict:
    arg_keys = jax.random.split(jax.random.key(seed), 2)
    part_splits = jax.random.split(jax.random.fold_in(arg_keys[1], part), 2)
    snapshots = normal_values(part_splits[0], (TIMES * LAT, LON), 1.0, 6.0, ((0, 16),), jnp.float32)
    return {"snapshots": snapshots}


def basis_matrix(times):
    steps = jnp.arange(times).astype(jnp.float32)
    columns = [jnp.ones_like(steps), (steps - (times - 1) / 2.0) / (times / 2.0)]
    for harmonic in range(1, 7):
        columns.append(jnp.cos(2.0 * jnp.pi * harmonic * steps / 12.0))
    for harmonic in range(1, 6):
        columns.append(jnp.sin(2.0 * jnp.pi * harmonic * steps / 12.0))
    columns.append(jnp.cos(2.0 * jnp.pi * steps / times))
    columns.append(jnp.sin(2.0 * jnp.pi * steps / times))
    columns.append(jnp.cos(4.0 * jnp.pi * steps / times))
    return jnp.stack(columns, axis=1)

def projector_of(basis):
    gram = jnp.dot(basis.T, basis, precision=lax.Precision.HIGHEST)
    factor = jnp.linalg.cholesky(gram)
    middle = lax.linalg.triangular_solve(factor, basis.T, left_side=True, lower=True)
    return lax.linalg.triangular_solve(factor, middle, left_side=True, lower=True, transpose_a=True)

def reference(snapshots):
    series = snapshots.reshape(TIMES, LAT * LON)
    basis = basis_matrix(TIMES)
    projector = projector_of(basis)
    coeffs = jnp.dot(projector, series, precision=lax.Precision.HIGHEST)
    fitted = jnp.dot(basis, coeffs, precision=lax.Precision.HIGHEST)
    resid = series - fitted
    variance = jnp.mean(resid * resid, axis=0)
    return (coeffs.reshape(HARM, LAT, LON), variance.reshape(LAT, LON))
```

```python
import functools

import jax
import jax.numpy as jnp
import numpy as np
from jax import lax
from jax.experimental import pallas as pl
from jax.experimental.pallas import tpu as pltpu
from jax.sharding import PartitionSpec as P

TIMES = 96
HARM = 16
MONTHS = 12
SPAN = 24
CHAIN = TIMES // SPAN
SLOW = 4
SUMS = MONTHS + SLOW + 1
LANES = 128
ROWS = 8
AHEAD = 8
MESH = pl.DeviceIdType.MESH


def fit_constants():
    steps = np.arange(TIMES, dtype=np.float64)
    slow = np.stack(
        [
            (steps - (TIMES - 1) / 2.0) / (TIMES / 2.0),
            np.cos(2.0 * np.pi * steps / TIMES),
            np.sin(2.0 * np.pi * steps / TIMES),
            np.cos(4.0 * np.pi * steps / TIMES),
        ],
        axis=1,
    )
    month = np.arange(MONTHS, dtype=np.float64)
    angles = 2.0 * np.pi * month / MONTHS
    periodic = [np.cos(j * angles) for j in range(7)] + [np.sin(j * angles) for j in range(1, 6)]
    unmix = np.linalg.inv(np.stack(periodic, axis=1))
    years = TIMES // MONTHS
    cross = slow.reshape(years, MONTHS, SLOW).sum(axis=0)
    inner = np.linalg.inv(slow.T @ slow - cross.T @ cross / years)
    return slow, cross, inner, unmix, years


def dot(weights, values):
    total = None
    for weight, value in zip(weights, values):
        term = value * np.float32(weight)
        total = term if total is None else total + term
    return total


def finish(sums):
    _, cross, inner, unmix, years = fit_constants()
    by_month, moments, squares = sums[:MONTHS], sums[MONTHS : MONTHS + SLOW], sums[-1]
    reduced = [moments[k] - dot(cross[:, k] / years, by_month) for k in range(SLOW)]
    slow = [dot(inner[k], reduced) for k in range(SLOW)]
    level = [(by_month[m] - dot(cross[m], slow)) * np.float32(1.0 / years) for m in range(MONTHS)]
    explained = slow[0] * moments[0]
    for k in range(1, SLOW):
        explained = explained + slow[k] * moments[k]
    for m in range(MONTHS):
        explained = explained + level[m] * by_month[m]
    half = MONTHS // 2
    even = [level[0]] + [level[m] + level[MONTHS - m] for m in range(1, half)] + [level[half]]
    odd = [level[m] - level[MONTHS - m] for m in range(1, half)]
    cosines = [dot(unmix[j, : half + 1], even) for j in range(half + 1)]
    sines = [dot(unmix[half + j, 1:half], odd) for j in range(1, half)]
    coeffs = [cosines[0], slow[0]] + cosines[1:] + sines + slow[1:]
    return coeffs, (squares - explained) * np.float32(1.0 / TIMES)


def kernel(
    groups, lat, local_rows,
    table, field, coeff_out, var_out,
    raw, part, below, above, done,
    raw_send, raw_recv, part_send, below_recv, above_recv, out_sem,
):
    members = groups // CHAIN
    chunks = lat // ROWS
    me = lax.axis_index("io")
    link, member = me // members, lax.rem(me, members)
    device = lambda at, who: {"io": at * members + who}

    barrier = pltpu.get_barrier_semaphore()
    for step in range(1, members):
        other = lax.rem(member + step, members)
        pl.semaphore_signal(barrier, inc=1, device_id=device(link, other), device_id_type=MESH)

    @pl.when(link > 0)
    def _():
        pl.semaphore_signal(barrier, inc=1, device_id=device(link - 1, member), device_id_type=MESH)

    @pl.when(link < CHAIN - 1)
    def _():
        pl.semaphore_signal(barrier, inc=1, device_id=device(link + 1, member), device_id_type=MESH)

    ends = (link == 0).astype(jnp.int32) + (link == CHAIN - 1).astype(jnp.int32)
    pl.semaphore_wait(barrier, members + 1 - ends)

    def spread_rows(chunk, row, count, time):
        for step in list(range(1, members)) + [0]:
            other = lax.rem(member + step, members)
            for to in range(CHAIN):
                lon = pl.multiple_of((to * members + other) * LANES, LANES)
                if count is None:
                    src = field.at[pl.ds(row, ROWS), pl.ds(lon, LANES)]
                    dst = raw.at[chunk, to, time]
                else:
                    src = field.at[:, pl.ds(row, ROWS), pl.ds(lon, LANES)]
                    dst = raw.at[chunk, to, pl.ds(time, count)]
                if step == 0:
                    pltpu.make_async_copy(src, dst, raw_recv.at[chunk]).start()
                else:
                    pltpu.make_async_remote_copy(
                        src_ref=src, dst_ref=dst, send_sem=raw_send, recv_sem=raw_recv.at[chunk],
                        device_id=device(link, other), device_id_type=MESH,
                    ).start()

    def spread(chunk):
        if local_rows % lat == 0:
            count = local_rows // lat
            spread_rows(chunk, pl.multiple_of(chunk * ROWS, ROWS), count, member * count)
        else:
            first = member * local_rows
            for extra in range(local_rows // lat + 2):
                time = first // lat + extra
                row = time * lat + chunk * ROWS - first

                @pl.when((row >= 0) & (row < local_rows))
                def _():
                    spread_rows(chunk, pl.multiple_of(row, ROWS), None, time)

    def send(chunk, to, up):
        pltpu.make_async_remote_copy(
            src_ref=part.at[chunk, to],
            dst_ref=(below if up else above).at[chunk, to],
            send_sem=part_send,
            recv_sem=(below_recv if up else above_recv).at[chunk, to],
            device_id=device(link + 1 if up else link - 1, member),
            device_id_type=MESH,
        ).start()

    def arrive(chunk, to, up):
        box, sem = (below, below_recv) if up else (above, above_recv)
        pltpu.make_async_copy(box.at[chunk, to], box.at[chunk, to], sem.at[chunk, to]).wait()
        for k in range(SUMS):
            part[chunk, to, k] = part[chunk, to, k] + box[chunk, to, k]

    def add_up(chunk):
        pltpu.make_async_copy(raw.at[chunk], raw.at[chunk], raw_recv.at[chunk]).wait()
        moments = [[None] * (SLOW + 1) for _ in range(CHAIN)]
        for month in range(MONTHS):
            kept = [None] * CHAIN
            for time in range(month, SPAN, MONTHS):
                weights = [table[(link * SPAN + time) * SLOW + k] for k in range(SLOW)]
                for to in range(CHAIN):
                    value = raw[chunk, to, time]
                    kept[to] = value if kept[to] is None else kept[to] + value
                    terms = [value * weight for weight in weights] + [value * value]
                    own = moments[to]
                    for k, term in enumerate(terms):
                        own[k] = term if own[k] is None else own[k] + term
            for to in range(CHAIN):
                part[chunk, to, month] = kept[to]
        for to in range(CHAIN):
            for k in range(SLOW + 1):
                part[chunk, to, MONTHS + k] = moments[to][k]

        @pl.when(link == 0)
        def _():
            for to in range(CHAIN - 1, 0, -1):
                send(chunk, to, True)

        @pl.when(link == CHAIN - 1)
        def _():
            for to in range(CHAIN - 1):
                send(chunk, to, False)

    def relay(step):
        for at in range(1, CHAIN - 1):

            @pl.when((link == at) & (step >= at) & (step < chunks + at))
            def _():
                for to in range(CHAIN - 1, at, -1):
                    arrive(step - at, to, True)
                    send(step - at, to, True)

            lag = CHAIN - 1 - at

            @pl.when((link == at) & (step >= lag) & (step < chunks + lag))
            def _():
                for to in range(at):
                    arrive(step - lag, to, False)
                    send(step - lag, to, False)

    def close(chunk):
        @pl.when(link > 0)
        def _():
            arrive(chunk, link, True)

        @pl.when(link < CHAIN - 1)
        def _():
            arrive(chunk, link, False)

        coeffs, variance = finish([part[chunk, link, k] for k in range(SUMS)])
        for k in range(HARM):
            done[chunk, k] = coeffs[k]
        done[chunk, HARM] = variance
        rows = pl.ds(pl.multiple_of(chunk * ROWS, ROWS), ROWS)
        pltpu.make_async_copy(done.at[chunk, pl.ds(0, HARM)], coeff_out.at[:, rows, :], out_sem.at[0]).start()
        pltpu.make_async_copy(done.at[chunk, HARM], var_out.at[rows, :], out_sem.at[1]).start()

    lag = CHAIN + 1
    lax.fori_loop(0, min(AHEAD, chunks), lambda c, _: (spread(c), 0)[1], 0)

    def body(step, carry):
        @pl.when(step + AHEAD < chunks)
        def _():
            spread(step + AHEAD)

        @pl.when(step < chunks)
        def _():
            add_up(step)

        relay(step)

        @pl.when(step >= lag)
        def _():
            close(step - lag)

        return carry

    lax.fori_loop(0, chunks + lag, body, 0)

    lons = pl.ds(0, (members - 1) * CHAIN * LANES)
    sent = field.at[:, :, lons] if local_rows % lat == 0 else field.at[:, lons]
    pltpu.make_async_copy(sent, sent, raw_send).wait()
    passed = part.at[:, pl.ds(0, CHAIN - 1)]
    pltpu.make_async_copy(passed, passed, part_send).wait()
    pltpu.make_async_copy(coeff_out, coeff_out, out_sem.at[0]).wait()
    pltpu.make_async_copy(var_out, var_out, out_sem.at[1]).wait()


def local(snapshots):
    groups = lax.axis_size("io")
    local_rows, width = snapshots.shape
    lat = local_rows * groups // TIMES
    if width != groups * LANES or lat % ROWS or local_rows % ROWS or groups % CHAIN:
        raise ValueError("unsupported sizes")
    chunks = lat // ROWS
    slow = fit_constants()[0]
    table = jnp.asarray(slow.reshape(-1), jnp.float32)
    field = snapshots.reshape(local_rows // lat, lat, width) if local_rows % lat == 0 else snapshots
    return pl.pallas_call(
        functools.partial(kernel, groups, lat, local_rows),
        out_shape=(
            jax.ShapeDtypeStruct((HARM, lat, LANES), jnp.float32),
            jax.ShapeDtypeStruct((lat, LANES), jnp.float32),
        ),
        in_specs=[pl.BlockSpec(memory_space=pltpu.SMEM), pl.BlockSpec(memory_space=pl.ANY)],
        out_specs=(pl.BlockSpec(memory_space=pl.ANY), pl.BlockSpec(memory_space=pl.ANY)),
        scratch_shapes=[
            pltpu.VMEM((chunks, CHAIN, SPAN, ROWS, LANES), jnp.float32),
            pltpu.VMEM((chunks, CHAIN, SUMS, ROWS, LANES), jnp.float32),
            pltpu.VMEM((chunks, CHAIN, SUMS, ROWS, LANES), jnp.float32),
            pltpu.VMEM((chunks, CHAIN, SUMS, ROWS, LANES), jnp.float32),
            pltpu.VMEM((chunks, SUMS, ROWS, LANES), jnp.float32),
            pltpu.SemaphoreType.DMA,
            pltpu.SemaphoreType.DMA((chunks,)),
            pltpu.SemaphoreType.DMA,
            pltpu.SemaphoreType.DMA((chunks, CHAIN)),
            pltpu.SemaphoreType.DMA((chunks, CHAIN)),
            pltpu.SemaphoreType.DMA((2,)),
        ],
        compiler_params=pltpu.CompilerParams(
            collective_id=0, has_side_effects=True, vmem_limit_bytes=56 * 2**20
        ),
        name="climatology",
    )(table, field)


def solution(mesh):
    return jax.shard_map(
        local,
        mesh=mesh,
        in_specs=(P(("rep", "io"), None),),
        out_specs=(P("rep", None, "io"), P("rep", "io")),
        check_vma=False,
    )
```

```python
import functools

import jax
import jax.numpy as jnp
import numpy as np
from jax import lax
from jax.experimental import pallas as pl
from jax.experimental.pallas import tpu as pltpu
from jax.sharding import PartitionSpec as P

TIMES = 96
HARM = 16
MONTHS = 12
SPAN = 24
CHAIN = TIMES // SPAN
SLOW = 4
SUMS = MONTHS + SLOW + 1
LANES = 128
ROWS = 8
AHEAD = 8
CLOSE_LAG = 3
MESH = pl.DeviceIdType.MESH


def fit_constants():
    steps = np.arange(TIMES, dtype=np.float64)
    slow = np.stack(
        [
            (steps - (TIMES - 1) / 2.0) / (TIMES / 2.0),
            np.cos(2.0 * np.pi * steps / TIMES),
            np.sin(2.0 * np.pi * steps / TIMES),
            np.cos(4.0 * np.pi * steps / TIMES),
        ],
        axis=1,
    )
    month = np.arange(MONTHS, dtype=np.float64)
    angles = 2.0 * np.pi * month / MONTHS
    periodic = [np.cos(j * angles) for j in range(7)] + [np.sin(j * angles) for j in range(1, 6)]
    unmix = np.linalg.inv(np.stack(periodic, axis=1))
    years = TIMES // MONTHS
    cross = slow.reshape(years, MONTHS, SLOW).sum(axis=0)
    inner = np.linalg.inv(slow.T @ slow - cross.T @ cross / years)
    return slow, cross, inner, unmix, years


def dot(weights, values):
    total = None
    for weight, value in zip(weights, values):
        term = value * np.float32(weight)
        total = term if total is None else total + term
    return total


def finish(sums):
    _, cross, inner, unmix, years = fit_constants()
    by_month, moments, squares = sums[:MONTHS], sums[MONTHS : MONTHS + SLOW], sums[-1]
    reduced = [moments[k] - dot(cross[:, k] / years, by_month) for k in range(SLOW)]
    slow = [dot(inner[k], reduced) for k in range(SLOW)]
    level = [(by_month[m] - dot(cross[m], slow)) * np.float32(1.0 / years) for m in range(MONTHS)]
    explained = slow[0] * moments[0]
    for k in range(1, SLOW):
        explained = explained + slow[k] * moments[k]
    for m in range(MONTHS):
        explained = explained + level[m] * by_month[m]
    half = MONTHS // 2
    even = [level[0]] + [level[m] + level[MONTHS - m] for m in range(1, half)] + [level[half]]
    odd = [level[m] - level[MONTHS - m] for m in range(1, half)]
    cosines = [dot(unmix[j, : half + 1], even) for j in range(half + 1)]
    sines = [dot(unmix[half + j, 1:half], odd) for j in range(1, half)]
    coeffs = [cosines[0], slow[0]] + cosines[1:] + sines + slow[1:]
    return coeffs, (squares - explained) * np.float32(1.0 / TIMES)


def kernel(
    groups, lat, local_rows,
    table, field, coeff_out, var_out,
    raw, part, below, above,
    raw_send, raw_recv, part_send, below_recv, above_recv,
):
    members = groups // CHAIN
    chunks = lat // ROWS
    me = lax.axis_index("io")
    link, member = me // members, lax.rem(me, members)
    device = lambda at, who: {"io": at * members + who}

    barrier = pltpu.get_barrier_semaphore()
    for step in range(1, members):
        other = lax.rem(member + step, members)
        pl.semaphore_signal(barrier, inc=1, device_id=device(link, other), device_id_type=MESH)

    @pl.when(link > 0)
    def _():
        pl.semaphore_signal(barrier, inc=1, device_id=device(link - 1, member), device_id_type=MESH)

    @pl.when(link < CHAIN - 1)
    def _():
        pl.semaphore_signal(barrier, inc=1, device_id=device(link + 1, member), device_id_type=MESH)

    ends = (link == 0).astype(jnp.int32) + (link == CHAIN - 1).astype(jnp.int32)
    pl.semaphore_wait(barrier, members + 1 - ends)

    def block_at(rank):
        orders = []
        for at in range(CHAIN):
            up, down = list(range(CHAIN - 1, at, -1)), list(range(at))
            orders.append((up + down if len(up) >= len(down) else down + up) + [at])
        return sum((link == at).astype(jnp.int32) * orders[at][rank] for at in range(CHAIN))

    def spread_rows(chunk, to, row, count, time):
        for step in list(range(1, members)) + [0]:
            other = lax.rem(member + step, members)
            lon = pl.multiple_of((to * members + other) * LANES, LANES)
            if count is None:
                src = field.at[pl.ds(row, ROWS), pl.ds(lon, LANES)]
                dst = raw.at[chunk, to, time]
            else:
                src = field.at[:, pl.ds(row, ROWS), pl.ds(lon, LANES)]
                dst = raw.at[chunk, to, pl.ds(time, count)]
            if step == 0:
                pltpu.make_async_copy(src, dst, raw_recv.at[chunk, to]).start()
            else:
                pltpu.make_async_remote_copy(
                    src_ref=src, dst_ref=dst, send_sem=raw_send, recv_sem=raw_recv.at[chunk, to],
                    device_id=device(link, other), device_id_type=MESH,
                ).start()

    def spread_block(chunk, to):
        if local_rows % lat == 0:
            count = local_rows // lat
            spread_rows(chunk, to, pl.multiple_of(chunk * ROWS, ROWS), count, member * count)
        else:
            first = member * local_rows
            for extra in range(local_rows // lat + 2):
                time = first // lat + extra
                row = time * lat + chunk * ROWS - first

                @pl.when((row >= 0) & (row < local_rows))
                def _():
                    spread_rows(chunk, to, pl.multiple_of(row, ROWS), None, time)

    def each(step, act):
        for rank in range(CHAIN):

            @pl.when((step >= rank) & (step < chunks + rank))
            def _():
                act(step - rank, block_at(rank))

    def send(chunk, to, up):
        pltpu.make_async_remote_copy(
            src_ref=part.at[chunk, to],
            dst_ref=(below if up else above).at[chunk, to],
            send_sem=part_send,
            recv_sem=(below_recv if up else above_recv).at[chunk, to],
            device_id=device(link + 1 if up else link - 1, member),
            device_id_type=MESH,
        ).start()

    def arrive(chunk, to, up):
        box, sem = (below, below_recv) if up else (above, above_recv)
        pltpu.make_async_copy(box.at[chunk, to], box.at[chunk, to], sem.at[chunk, to]).wait()
        for k in range(SUMS):
            part[chunk, to, k] = part[chunk, to, k] + box[chunk, to, k]

    def add_up(chunk, to):
        pltpu.make_async_copy(raw.at[chunk, to], raw.at[chunk, to], raw_recv.at[chunk, to]).wait()
        moments = [None] * (SLOW + 1)
        for month in range(MONTHS):
            kept = None
            for time in range(month, SPAN, MONTHS):
                value = raw[chunk, to, time]
                kept = value if kept is None else kept + value
                terms = [value * table[(link * SPAN + time) * SLOW + k] for k in range(SLOW)] + [value * value]
                moments = [term if own is None else own + term for own, term in zip(moments, terms)]
            part[chunk, to, month] = kept
        for k in range(SLOW + 1):
            part[chunk, to, MONTHS + k] = moments[k]

        @pl.when((link == 0) & (to > 0))
        def _():
            send(chunk, to, True)

        @pl.when((link == CHAIN - 1) & (to < CHAIN - 1))
        def _():
            send(chunk, to, False)

    def relay(step):
        for at in range(1, CHAIN - 1):
            for to in range(CHAIN - 1, at, -1):
                lag = CHAIN - 1 - to + at

                @pl.when((link == at) & (step >= lag) & (step < chunks + lag))
                def _():
                    arrive(step - lag, to, True)
                    send(step - lag, to, True)

            for to in range(at):
                lag = to + CHAIN - 1 - at

                @pl.when((link == at) & (step >= lag) & (step < chunks + lag))
                def _():
                    arrive(step - lag, to, False)
                    send(step - lag, to, False)

    def close(chunk):
        @pl.when(link > 0)
        def _():
            arrive(chunk, link, True)

        @pl.when(link < CHAIN - 1)
        def _():
            arrive(chunk, link, False)

        coeffs, variance = finish([part[chunk, link, k] for k in range(SUMS)])
        rows = pl.ds(pl.multiple_of(chunk * ROWS, ROWS), ROWS)
        for k in range(HARM):
            coeff_out[k, rows, :] = coeffs[k]
        var_out[rows, :] = variance

    ramp = CHAIN - 1
    lax.fori_loop(0, AHEAD, lambda step, _: (each(step, spread_block), 0)[1], 0)

    def body(step, carry):
        each(step + AHEAD, spread_block)
        each(step, add_up)
        relay(step)

        @pl.when(step >= ramp + CLOSE_LAG)
        def _():
            close(step - ramp - CLOSE_LAG)

        return carry

    lax.fori_loop(0, chunks + ramp + CLOSE_LAG, body, 0)

    lons = pl.ds(0, (members - 1) * CHAIN * LANES)
    sent = field.at[:, :, lons] if local_rows % lat == 0 else field.at[:, lons]
    pltpu.make_async_copy(sent, sent, raw_send).wait()
    passed = part.at[:, pl.ds(0, CHAIN - 1)]
    pltpu.make_async_copy(passed, passed, part_send).wait()


def local(snapshots):
    groups = lax.axis_size("io")
    local_rows, width = snapshots.shape
    lat = local_rows * groups // TIMES
    if width != groups * LANES or lat % ROWS or local_rows % ROWS or groups % CHAIN:
        raise ValueError("unsupported sizes")
    chunks = lat // ROWS
    slow = fit_constants()[0]
    table = jnp.asarray(slow.reshape(-1), jnp.float32)
    field = snapshots.reshape(local_rows // lat, lat, width) if local_rows % lat == 0 else snapshots
    return pl.pallas_call(
        functools.partial(kernel, groups, lat, local_rows),
        out_shape=(
            jax.ShapeDtypeStruct((HARM, lat, LANES), jnp.float32),
            jax.ShapeDtypeStruct((lat, LANES), jnp.float32),
        ),
        in_specs=[pl.BlockSpec(memory_space=pltpu.SMEM), pl.BlockSpec(memory_space=pl.ANY)],
        out_specs=(pl.BlockSpec(memory_space=pltpu.VMEM), pl.BlockSpec(memory_space=pltpu.VMEM)),
        scratch_shapes=[
            pltpu.VMEM((chunks, CHAIN, SPAN, ROWS, LANES), jnp.float32),
            pltpu.VMEM((chunks, CHAIN, SUMS, ROWS, LANES), jnp.float32),
            pltpu.VMEM((chunks, CHAIN, SUMS, ROWS, LANES), jnp.float32),
            pltpu.VMEM((chunks, CHAIN, SUMS, ROWS, LANES), jnp.float32),
            pltpu.SemaphoreType.DMA,
            pltpu.SemaphoreType.DMA((chunks, CHAIN)),
            pltpu.SemaphoreType.DMA,
            pltpu.SemaphoreType.DMA((chunks, CHAIN)),
            pltpu.SemaphoreType.DMA((chunks, CHAIN)),
        ],
        compiler_params=pltpu.CompilerParams(
            collective_id=0, has_side_effects=True, vmem_limit_bytes=44 * 2**20
        ),
        name="climatology",
    )(table, field)


def solution(mesh):
    return jax.shard_map(
        local,
        mesh=mesh,
        in_specs=(P(("rep", "io"), None),),
        out_specs=(P("rep", None, "io"), P("rep", "io")),
        check_vma=False,
    )
```

```python
import functools

import jax
import jax.numpy as jnp
import numpy as np
from jax import lax
from jax.experimental import pallas as pl
from jax.experimental.pallas import tpu as pltpu
from jax.sharding import PartitionSpec as P

TIMES = 96
HARM = 16
MONTHS = 12
SPAN = 24
CHAIN = TIMES // SPAN
SLOW = 4
SUMS = MONTHS + SLOW + 1
LANES = 128
ROWS = 8
AHEAD = 8
CLOSE_LAG = 3
MESH = pl.DeviceIdType.MESH


def fit_constants():
    steps = np.arange(TIMES, dtype=np.float64)
    slow = np.stack(
        [
            (steps - (TIMES - 1) / 2.0) / (TIMES / 2.0),
            np.cos(2.0 * np.pi * steps / TIMES),
            np.sin(2.0 * np.pi * steps / TIMES),
            np.cos(4.0 * np.pi * steps / TIMES),
        ],
        axis=1,
    )
    month = np.arange(MONTHS, dtype=np.float64)
    angles = 2.0 * np.pi * month / MONTHS
    periodic = [np.cos(j * angles) for j in range(7)] + [np.sin(j * angles) for j in range(1, 6)]
    unmix = np.linalg.inv(np.stack(periodic, axis=1))
    years = TIMES // MONTHS
    cross = slow.reshape(years, MONTHS, SLOW).sum(axis=0)
    inner = np.linalg.inv(slow.T @ slow - cross.T @ cross / years)
    return slow, cross, inner, unmix, years


def dot(weights, values):
    total = None
    for weight, value in zip(weights, values):
        term = value * np.float32(weight)
        total = term if total is None else total + term
    return total


def finish(sums):
    _, cross, inner, unmix, years = fit_constants()
    by_month, moments, squares = sums[:MONTHS], sums[MONTHS : MONTHS + SLOW], sums[-1]
    reduced = [moments[k] - dot(cross[:, k] / years, by_month) for k in range(SLOW)]
    slow = [dot(inner[k], reduced) for k in range(SLOW)]
    level = [(by_month[m] - dot(cross[m], slow)) * np.float32(1.0 / years) for m in range(MONTHS)]
    explained = slow[0] * moments[0]
    for k in range(1, SLOW):
        explained = explained + slow[k] * moments[k]
    for m in range(MONTHS):
        explained = explained + level[m] * by_month[m]
    half = MONTHS // 2
    even = [level[0]] + [level[m] + level[MONTHS - m] for m in range(1, half)] + [level[half]]
    odd = [level[m] - level[MONTHS - m] for m in range(1, half)]
    cosines = [dot(unmix[j, : half + 1], even) for j in range(half + 1)]
    sines = [dot(unmix[half + j, 1:half], odd) for j in range(1, half)]
    coeffs = [cosines[0], slow[0]] + cosines[1:] + sines + slow[1:]
    return coeffs, (squares - explained) * np.float32(1.0 / TIMES)


def kernel(
    groups, lat, local_rows,
    field, coeff_out, var_out,
    raw, part, below, above,
    raw_send, raw_recv, part_send, below_recv, above_recv,
):
    members = groups // CHAIN
    chunks = lat // ROWS
    me = lax.axis_index("io")
    link, member = me // members, lax.rem(me, members)
    device = lambda at, who: {"io": at * members + who}

    span = fit_constants()[0][:SPAN]
    offset = link.astype(jnp.float32) * np.float32(SPAN / (TIMES / 2.0))
    quarter = lambda at: (link == at).astype(jnp.float32)
    turn_cos, turn_sin = quarter(0) - quarter(2), quarter(1) - quarter(3)
    flip = quarter(0) - quarter(1) + quarter(2) - quarter(3)

    barrier = pltpu.get_barrier_semaphore()
    for step in range(1, members):
        other = lax.rem(member + step, members)
        pl.semaphore_signal(barrier, inc=1, device_id=device(link, other), device_id_type=MESH)

    @pl.when(link > 0)
    def _():
        pl.semaphore_signal(barrier, inc=1, device_id=device(link - 1, member), device_id_type=MESH)

    @pl.when(link < CHAIN - 1)
    def _():
        pl.semaphore_signal(barrier, inc=1, device_id=device(link + 1, member), device_id_type=MESH)

    ends = (link == 0).astype(jnp.int32) + (link == CHAIN - 1).astype(jnp.int32)
    pl.semaphore_wait(barrier, members + 1 - ends)

    def block_at(rank):
        orders = []
        for at in range(CHAIN):
            up, down = list(range(CHAIN - 1, at, -1)), list(range(at))
            orders.append((up + down if len(up) >= len(down) else down + up) + [at])
        return sum((link == at).astype(jnp.int32) * orders[at][rank] for at in range(CHAIN))

    def spread_rows(chunk, to, row, count, time):
        for step in list(range(1, members)) + [0]:
            other = lax.rem(member + step, members)
            lon = pl.multiple_of((to * members + other) * LANES, LANES)
            if count is None:
                src = field.at[pl.ds(row, ROWS), pl.ds(lon, LANES)]
                dst = raw.at[chunk, to, time]
            else:
                src = field.at[:, pl.ds(row, ROWS), pl.ds(lon, LANES)]
                dst = raw.at[chunk, to, pl.ds(time, count)]
            if step == 0:
                pltpu.make_async_copy(src, dst, raw_recv.at[chunk, to]).start()
            else:
                pltpu.make_async_remote_copy(
                    src_ref=src, dst_ref=dst, send_sem=raw_send, recv_sem=raw_recv.at[chunk, to],
                    device_id=device(link, other), device_id_type=MESH,
                ).start()

    def spread_block(chunk, to):
        if local_rows % lat == 0:
            count = local_rows // lat
            spread_rows(chunk, to, pl.multiple_of(chunk * ROWS, ROWS), count, member * count)
        else:
            first = member * local_rows
            for extra in range(local_rows // lat + 2):
                time = first // lat + extra
                row = time * lat + chunk * ROWS - first

                @pl.when((row >= 0) & (row < local_rows))
                def _():
                    spread_rows(chunk, to, pl.multiple_of(row, ROWS), None, time)

    def each(step, act):
        for rank in range(CHAIN):

            @pl.when((step >= rank) & (step < chunks + rank))
            def _():
                act(step - rank, block_at(rank))

    def send(chunk, to, up):
        pltpu.make_async_remote_copy(
            src_ref=part.at[chunk, to],
            dst_ref=(below if up else above).at[chunk, to],
            send_sem=part_send,
            recv_sem=(below_recv if up else above_recv).at[chunk, to],
            device_id=device(link + 1 if up else link - 1, member),
            device_id_type=MESH,
        ).start()

    def arrive(chunk, to, up):
        box, sem = (below, below_recv) if up else (above, above_recv)
        pltpu.make_async_copy(box.at[chunk, to], box.at[chunk, to], sem.at[chunk, to]).wait()
        for k in range(SUMS):
            part[chunk, to, k] = part[chunk, to, k] + box[chunk, to, k]

    def add_up(chunk, to):
        pltpu.make_async_copy(raw.at[chunk, to], raw.at[chunk, to], raw_recv.at[chunk, to]).wait()
        local = [None] * (SLOW + 1)
        whole = None
        for month in range(MONTHS):
            kept = None
            for time in range(month, SPAN, MONTHS):
                value = raw[chunk, to, time]
                kept = value if kept is None else kept + value
                terms = [value * np.float32(span[time, k]) for k in range(SLOW)] + [value * value]
                local = [term if own is None else own + term for own, term in zip(local, terms)]
            part[chunk, to, month] = kept
            whole = kept if whole is None else whole + kept
        trend, cosine, sine, double, squares = local
        part[chunk, to, MONTHS] = trend + whole * offset
        part[chunk, to, MONTHS + 1] = cosine * turn_cos - sine * turn_sin
        part[chunk, to, MONTHS + 2] = cosine * turn_sin + sine * turn_cos
        part[chunk, to, MONTHS + 3] = double * flip
        part[chunk, to, MONTHS + 4] = squares

        @pl.when((link == 0) & (to > 0))
        def _():
            send(chunk, to, True)

        @pl.when((link == CHAIN - 1) & (to < CHAIN - 1))
        def _():
            send(chunk, to, False)

    def relay(step):
        for at in range(1, CHAIN - 1):
            for to in range(CHAIN - 1, at, -1):
                lag = CHAIN - 1 - to + at

                @pl.when((link == at) & (step >= lag) & (step < chunks + lag))
                def _():
                    arrive(step - lag, to, True)
                    send(step - lag, to, True)

            for to in range(at):
                lag = to + CHAIN - 1 - at

                @pl.when((link == at) & (step >= lag) & (step < chunks + lag))
                def _():
                    arrive(step - lag, to, False)
                    send(step - lag, to, False)

    def close(chunk):
        @pl.when(link > 0)
        def _():
            arrive(chunk, link, True)

        @pl.when(link < CHAIN - 1)
        def _():
            arrive(chunk, link, False)

        coeffs, variance = finish([part[chunk, link, k] for k in range(SUMS)])
        rows = pl.ds(pl.multiple_of(chunk * ROWS, ROWS), ROWS)
        for k in range(HARM):
            coeff_out[k, rows, :] = coeffs[k]
        var_out[rows, :] = variance

    ramp = CHAIN - 1
    lax.fori_loop(0, AHEAD, lambda step, _: (each(step, spread_block), 0)[1], 0)

    def body(step, carry):
        each(step + AHEAD, spread_block)
        each(step, add_up)
        relay(step)

        @pl.when(step >= ramp + CLOSE_LAG)
        def _():
            close(step - ramp - CLOSE_LAG)

        return carry

    lax.fori_loop(0, chunks + ramp + CLOSE_LAG, body, 0)

    lons = pl.ds(0, (members - 1) * CHAIN * LANES)
    sent = field.at[:, :, lons] if local_rows % lat == 0 else field.at[:, lons]
    pltpu.make_async_copy(sent, sent, raw_send).wait()
    passed = part.at[:, pl.ds(0, CHAIN - 1)]
    pltpu.make_async_copy(passed, passed, part_send).wait()


def put_out(coeffs, variance, coeff_out, var_out, sem):
    copies = [
        pltpu.make_async_copy(coeffs, coeff_out, sem.at[0]),
        pltpu.make_async_copy(variance, var_out, sem.at[1]),
    ]
    for copy in copies:
        copy.start()
    for copy in copies:
        copy.wait()


def local(snapshots):
    groups = lax.axis_size("io")
    local_rows, width = snapshots.shape
    lat = local_rows * groups // TIMES
    if width != groups * LANES or lat % ROWS or local_rows % ROWS or groups % CHAIN:
        raise ValueError("unsupported sizes")
    chunks = lat // ROWS
    field = snapshots.reshape(local_rows // lat, lat, width) if local_rows % lat == 0 else snapshots
    results = pl.pallas_call(
        functools.partial(kernel, groups, lat, local_rows),
        out_shape=(
            jax.ShapeDtypeStruct((HARM, lat, LANES), jnp.float32),
            jax.ShapeDtypeStruct((lat, LANES), jnp.float32),
        ),
        in_specs=[pl.BlockSpec(memory_space=pl.ANY)],
        out_specs=(pl.BlockSpec(memory_space=pltpu.VMEM), pl.BlockSpec(memory_space=pltpu.VMEM)),
        scratch_shapes=[
            pltpu.VMEM((chunks, CHAIN, SPAN, ROWS, LANES), jnp.float32),
            pltpu.VMEM((chunks, CHAIN, SUMS, ROWS, LANES), jnp.float32),
            pltpu.VMEM((chunks, CHAIN, SUMS, ROWS, LANES), jnp.float32),
            pltpu.VMEM((chunks, CHAIN, SUMS, ROWS, LANES), jnp.float32),
            pltpu.SemaphoreType.DMA,
            pltpu.SemaphoreType.DMA((chunks, CHAIN)),
            pltpu.SemaphoreType.DMA,
            pltpu.SemaphoreType.DMA((chunks, CHAIN)),
            pltpu.SemaphoreType.DMA((chunks, CHAIN)),
        ],
        compiler_params=pltpu.CompilerParams(
            collective_id=0, has_side_effects=True, vmem_limit_bytes=44 * 2**20
        ),
        name="climatology",
    )(field)
    return pl.pallas_call(
        put_out,
        out_shape=tuple(jax.ShapeDtypeStruct(r.shape, r.dtype) for r in results),
        in_specs=[pl.BlockSpec(memory_space=pltpu.VMEM)] * 2,
        out_specs=(pl.BlockSpec(memory_space=pl.ANY),) * 2,
        scratch_shapes=[pltpu.SemaphoreType.DMA((2,))],
        compiler_params=pltpu.CompilerParams(vmem_limit_bytes=4 * 2**20),
        name="put_out",
    )(*results)


def solution(mesh):
    return jax.shard_map(
        local,
        mesh=mesh,
        in_specs=(P(("rep", "io"), None),),
        out_specs=(P("rep", None, "io"), P("rep", "io")),
        check_vma=False,
    )
```
